32 devices in a mesh: dp: 8 (over y, x, core), mp: 4 (over z).
Axes of the slice: x: 2, y: 2, z: 4, core: 2. Of those that a mesh axis runs over, the one named last changes fastest.
Arguments:
- tokens: bfloat16 [1024, 8192], P(('dp', 'mp')), parts along dimension 0, may hold values from -6 to 6
- norm_gain: float32 [8192], replicated, may hold values from 0.5 to 1.5
- qkv_weight: bfloat16 [8192, 10240], P(None, 'mp'), may hold values from -0.0625 to 0.0625
- qkv_bias: float32 [10240], P('mp'), may hold values from -3 to 3
- qkv_grad: bfloat16 [1024, 10240], P('dp', 'mp'), parts along dimension 0, may hold values from -6 to 6
Outputs:
- qkv: bfloat16 [1024, 10240], P('dp', 'mp'), parts along dimension 0
- tokens_grad: float32 [1024, 8192], P(('dp', 'mp')), parts along dimension 0
- gain_grad: float32 [65536], P('dp'), parts along dimension 0
- bias_grad: float32 [81920], P(('dp', 'mp')), parts along dimension 0
The draws below stay inside these ranges and needn't reach their ends.
There are 8 independent parts, one for each index of `dp`. The reference program is written for one: setup_inputs(seed, part) draws one part's arguments, and reference() takes and returns one part's arrays. A program takes and returns all parts, laid end to end along the dimension named above; an argument that names none is the same for every part. Nothing has to cross between parts.
All inputs are finite; a program needn't handle non-finite values.
Results may differ from the reference program's by a relative error of at most 0.0046.
Values may be sent and summed in bfloat16 or wider, within the bound.
A program may use at most 128 MiB of HBM per device.

```python
import jax
import jax.numpy as jnp
from jax import lax

D = 8192
HEAD_DIM = 128
GROUP = 10
COLS = 10240
STRIDE = 8192
TOK_DEV = 32
TOKENS = 128


def strengthened(values, own_key, source, target, shards_of, factor):
    def block_of(axis_at):
        return (jnp.arange(values.shape[axis_at]) // (values.shape[axis_at] // shards_of)).reshape((-1,) + (1,) * (values.ndim - 1 - axis_at))

    first = jax.random.permutation(own_key, shards_of)[block_of(target)]
    far = (block_of(target) + shards_of // 2) % shards_of
    return jnp.where((block_of(source) == first) | (block_of(source) == far), factor * values, values)


def shard_levels(stream_key, shape, cuts, smallest, top_value):
    def one(axis_at, blocks):
        heights = jax.random.uniform(jax.random.fold_in(jax.random.fold_in(stream_key, 6), axis_at), (blocks,), jnp.float32, smallest / len(cuts), top_value / len(cuts))
        return jnp.repeat(jnp.exp(heights), shape[axis_at] // blocks).reshape((-1,) + (1,) * (len(shape) - axis_at - 1))

    factor_of = one(*cuts[0])
    for cut in cuts[1:]:
        factor_of = factor_of * one(*cut)
    return factor_of


def gaussian(own_key, dims, deviation, bound, shards=(), kind=jnp.bfloat16):
    array = deviation * jax.random.normal(own_key, dims, jnp.float32)
    if shards:
        array = array * shard_levels(own_key, dims, shards, -0.22, 0.18)
    return jnp.clip(array, -bound, bound).astype(kind)


def gaussian_with(stream_key, extent, deviation, limit, cuts, heavy, kind=jnp.bfloat16):
    array = deviation * jax.random.normal(stream_key, extent, jnp.float32)
    if cuts:
        array = array * shard_levels(stream_key, extent, cuts, -0.22, 0.18)
    return jnp.clip(strengthened(array, jax.random.fold_in(stream_key, 3), *heavy), -limit, limit).astype(kind)


def setup_inputs(seed: int = 0, part: int = 0) -> dict:
    key_list = jax.random.split(jax.random.key(seed), 6)
    part_keys = jax.random.split(jax.random.fold_in(key_list[5], part), 6)
    return {
        "tokens": gaussian(part_keys[0], (TOKENS, D), 1.0, 6.0, ((0, 4),)),
        "norm_gain": jnp.clip(1.0 + 0.1 * jax.random.normal(key_list[1], (D,), jnp.float32), 0.5, 1.5),
        "qkv_weight": gaussian(key_list[2], (D, COLS), D ** -0.5, 0.0625, ((1, 4),)),
        "qkv_bias": gaussian(key_list[3], (COLS,), 0.5, 3.0, ((0, 4),), jnp.float32),
        "qkv_grad": gaussian_with(part_keys[4], (TOKENS, COLS), 1.0, 6.0, ((1, 4),), (1, 0, 4, 2.0)),
    }


def rotate_heads(joined, first_col, position, sign):
    rows, cols = joined.shape
    heads = cols // HEAD_DIM
    half = HEAD_DIM // 2
    parts = joined.reshape(rows, heads, 2, half)
    inverse = jnp.exp(-jnp.log(jnp.float32(1000000.0)) * (2.0 * jnp.arange(half).astype(jnp.float32) / HEAD_DIM))
    angle = position.astype(jnp.float32)[:, None] * inverse[None, :]
    cosine = jnp.cos(angle)[:, None, :]
    sine = sign * jnp.sin(angle)[:, None, :]
    first = parts[:, :, 0, :]
    second = parts[:, :, 1, :]
    turned = jnp.stack([first * cosine - second * sine, second * cosine + first * sine], axis=2)
    head_index = first_col // HEAD_DIM + jnp.arange(heads)
    rotated = head_index % GROUP != GROUP - 1
    result = jnp.where(rotated[None, :, None, None], turned, parts)
    return result.reshape(rows, cols)

def reference(tokens, norm_gain, qkv_weight, qkv_bias, qkv_grad):
    row_index = jnp.arange(TOKENS).astype(jnp.int32)
    position = row_index // TOK_DEV * STRIDE + row_index % TOK_DEV
    values = tokens.astype(jnp.float32)
    scale = lax.rsqrt(lax.optimization_barrier(jnp.mean(values * values, axis=1, keepdims=True)) + 1e-06)
    normed = (values * scale * norm_gain[None, :]).astype(jnp.bfloat16)
    joined = jnp.dot(normed, qkv_weight, preferred_element_type=jnp.float32) + qkv_bias[None, :]
    qkv = rotate_heads(joined, 0, position, 1.0).astype(jnp.bfloat16)
    joined_grad = rotate_heads(qkv_grad.astype(jnp.float32), 0, position, -1.0)
    bias_grad = lax.optimization_barrier(jnp.sum(joined_grad, axis=0))
    joined_low = joined_grad.astype(jnp.bfloat16)
    normed_grad = lax.dot_general(joined_low, qkv_weight, (((1,), (1,)), ((), ())), preferred_element_type=jnp.float32)
    gain_grad = lax.optimization_barrier(jnp.sum(normed_grad * values * scale, axis=0))
    inner = lax.optimization_barrier(jnp.mean(norm_gain[None, :] * normed_grad * values, axis=1, keepdims=True))
    tokens_grad = scale * norm_gain[None, :] * normed_grad - values * scale * scale * scale * inner
    return (qkv, tokens_grad, gain_grad, bias_grad)
```

```python
import functools

import jax
import jax.numpy as jnp
import numpy as np
from jax import lax
from jax.experimental import pallas as pl
from jax.experimental.pallas import tpu as pltpu
from jax.sharding import PartitionSpec as P

HEAD_DIM = 128
SEQ_LEN = 32768
GROUP = 10
CHUNKS = 4
TILE_K = 512
PIECES = 4
MESH = pl.DeviceIdType.MESH


def rope_tables(rows, tok_dev, stride):
    half = HEAD_DIM // 2
    row = np.arange(rows)
    place = (row // tok_dev * stride + row % tok_dev).astype(np.float32)
    inverse = np.exp(
        -np.log(np.float32(1000000.0))
        * (np.float32(2.0) * np.arange(half).astype(np.float32) / np.float32(HEAD_DIM))
    ).astype(np.float32)
    angle = (place[:, None] * inverse[None, :]).astype(np.float32)
    cosine, sine = np.cos(angle).astype(np.float32), np.sin(angle).astype(np.float32)
    return np.concatenate([cosine, cosine], 1), np.concatenate([-sine, sine], 1)


def kernel(
    n,
    tok_h, gain_h, w_h, bias_h, grad_h, cos_h, sin_h,
    qkv, tgp, tok, weight, gg_ref, bg_ref,
    raw, gain, w, bias, grad, cos, sin,
    low, part, held, run, acc, square, scale_ref, gsum, gmine, gout, gin,
    tok_sem, in_sem, w_sem, send_sem, recv_sem, gsend_sem, grecv_sem, ready,
):
    me = lax.axis_index("mp")
    rows, depth = tok.shape
    width = w.shape[1]
    heads = width // HEAD_DIM
    span = depth // CHUNKS
    tiles = depth // TILE_K
    per = tiles // CHUNKS
    half = n // 2
    f32, bf16 = jnp.float32, jnp.bfloat16

    has_right, has_left = me < n - 1, me > 0
    ways = ((0, has_right, has_left), (1, has_left, has_right))
    barrier = pltpu.get_barrier_semaphore()

    def peer(way):
        return {"mp": lax.rem(me + (1 if way == 0 else n - 1), n)}

    @pl.when(has_right)
    def _():
        pl.semaphore_signal(barrier, inc=1, device_id=peer(0), device_id_type=MESH)

    def block(s):
        return pl.ds(pl.multiple_of(s * rows, rows), rows)

    def cols(c):
        return pl.ds(pl.multiple_of(c * span, span), span)

    def tok_copy(c):
        return pltpu.make_async_copy(
            tok_h.at[:, cols(c)], raw.at[block(me), cols(c)], tok_sem.at[c]
        )

    for c in range(CHUNKS):
        tok_copy(c).start()
    loads = []
    for i, (src, dst) in enumerate(
        ((gain_h, gain.at[0]), (grad_h, grad), (cos_h, cos), (sin_h, sin), (bias_h, bias.at[0]), (tok_h, tok))
    ):
        loads.append(pltpu.make_async_copy(src, dst, in_sem.at[i]))
        loads[i].start()

    def w_copy(i):
        k = pl.ds(pl.multiple_of(i * TILE_K, TILE_K), TILE_K)
        return pltpu.make_async_copy(w_h.at[k, :], w.at[k, :], w_sem.at[i])

    def transfer(way, buf, at, j, c):
        ref = buf.at[block(at), cols(c)]
        return pltpu.make_async_remote_copy(
            src_ref=ref,
            dst_ref=ref,
            send_sem=send_sem.at[way, j, c],
            recv_sem=recv_sem.at[way, j, c],
            device_id=peer(way),
            device_id_type=MESH,
        )

    def absorb(b, c):
        v = raw[block(b), cols(c)].astype(f32)
        held[block(b), cols(c)] = (v * gain[:, cols(c)]).astype(bf16)
        v = v * v
        while v.shape[1] > HEAD_DIM:
            m = v.shape[1] // 2
            v = v[:, :m] + v[:, m:]
        if isinstance(c, int):
            old = jnp.zeros_like(v) if c == 0 else square[block(b), :]
        else:
            old = jnp.where(c == 0, jnp.zeros_like(v), square[block(b), :])
        square[block(b), :] = old + v

    def settle(b):
        total = jnp.sum(square[block(b), :], axis=1, keepdims=True)
        scale_ref[block(b), :] = jnp.broadcast_to(lax.rsqrt(total / depth + 1e-06), (rows, HEAD_DIM))

    @pl.when(has_left)
    def _():
        pl.semaphore_wait(barrier, 1)
        pl.semaphore_signal(ready, inc=1, device_id=peer(1), device_id_type=MESH)

    for c in range(CHUNKS):
        tok_copy(c).wait()

        @pl.when(has_left)
        def _():
            transfer(1, raw, me, 0, c).start()

    @pl.loop(0, tiles)
    def _(i):
        w_copy(i).start()

    @pl.when(has_right)
    def _():
        pl.semaphore_wait(ready, 1)
        for c in range(CHUNKS):
            transfer(0, raw, me, 0, c).start()

    def arrive(j, c):
        for way, goes, comes in ways:
            @pl.when(comes)
            def _():
                transfer(way, raw, 0, j - 1, c).wait_recv()

    def prepare(j, c):
        for way, goes, comes in ways:
            back = me if way == 0 else n - 1 - me

            @pl.when(goes & (j > back))
            def _():
                t = n - j + me if way == 0 else j - n + me
                slot = t + 1 if way == 0 else t

                @pl.when(comes)
                def _():
                    value = part[block(t), cols(c)] + run[block(slot), cols(c)].astype(f32)
                    run[block(slot), cols(c)] = value.astype(bf16)

                @pl.when(jnp.logical_not(comes))
                def _():
                    run[block(slot), cols(c)] = part[block(t), cols(c)].astype(bf16)

    def launch(j, c):
        for way, goes, comes in ways:
            back = me if way == 0 else n - 1 - me

            @pl.when(goes & (j <= back))
            def _():
                transfer(way, raw, me - j if way == 0 else me + j, j, c).start()

            @pl.when(goes & (j > back))
            def _():
                t = n - j + me if way == 0 else j - n + me
                transfer(way, run, t + 1 if way == 0 else t, j, c).start()

    def take(j, c):
        for way, goes, comes in ways:
            back = me if way == 0 else n - 1 - me

            @pl.when(comes & (j <= back))
            def _():
                b = me - j if way == 0 else me + j
                absorb(b, c)
                if isinstance(c, int):
                    if c == CHUNKS - 1:
                        settle(b)
                else:
                    @pl.when(c == CHUNKS - 1)
                    def _():
                        settle(b)

    def step(j, c):
        arrive(j, c)
        prepare(j, c)
        launch(j, c)
        take(j, c)

    for l in loads[:5]:
        l.wait()
    for h in range(heads):
        hs = slice(h * HEAD_DIM, (h + 1) * HEAD_DIM)
        x = grad[:, hs].astype(f32)
        turned = x * cos[...] - pltpu.roll(x, HEAD_DIM // 2, 1) * sin[...]
        plain = lax.rem(me * heads + h, GROUP) == GROUP - 1
        x = jnp.where(plain, x, turned)
        bg_ref[:, hs] = jnp.sum(x, axis=0, keepdims=True)
        low[:, hs] = x.astype(bf16)

    def backward(c):
        @pl.loop(0, per)
        def _(i):
            at = c * per + i
            w_copy(at).wait()
            k = pl.ds(pl.multiple_of(at * TILE_K, TILE_K), TILE_K)
            part[:, k] = lax.dot_general(
                low[...], w[k, :], (((1,), (1,)), ((), ())), preferred_element_type=f32
            )

    @pl.loop(0, CHUNKS)
    def _(c):
        backward(c)
        absorb(me, c)

        @pl.when(c > 0)
        def _():
            step(1, c - 1)

    settle(me)
    step(1, CHUNKS - 1)

    @pl.loop(2, half)
    def _(j):
        @pl.loop(0, CHUNKS)
        def _(c):
            step(j, c)

    for c in range(CHUNKS - 1):
        step(half, c)
    arrive(half, CHUNKS - 1)
    prepare(half, CHUNKS - 1)
    take(half, CHUNKS - 1)

    def gain_add(t, slot):
        source = part if slot is None else run
        at = slice(t * rows, (t + 1) * rows) if slot is None else slice(slot * rows, (slot + 1) * rows)
        scale = scale_ref[t * rows:(t + 1) * rows, :]

        @pl.loop(0, depth // 1024)
        def _(i):
            for p in range(1024 // HEAD_DIM):
                k = pl.ds(pl.multiple_of(i * 1024 + p * HEAD_DIM, HEAD_DIM), HEAD_DIM)
                x = source[at, k].astype(f32) * raw[t * rows:(t + 1) * rows, k].astype(f32) * scale
                total = x[:8]
                for r in range(8, rows, 8):
                    total = total + x[r:r + 8]
                gsum[:, k] += total

    gsum[...] = jnp.zeros_like(gsum)
    for t in range(n):
        @pl.when((me - t < half) & (t - me < half))
        def _():
            gain_add(t, None)

        if t + half < n:
            @pl.when(me == t + half)
            def _():
                gain_add(t, t)
        if t - half >= 0:
            @pl.when(me == t - half)
            def _():
                gain_add(t, t + 1)
    piece = depth // 16
    for i in range(16):
        gmine[i:i + 1, :] = jnp.sum(gsum[:, i * piece:(i + 1) * piece], axis=0, keepdims=True)

    def gain_copy(way):
        return pltpu.make_async_remote_copy(
            src_ref=gout.at[way],
            dst_ref=gin.at[way],
            send_sem=gsend_sem.at[way],
            recv_sem=grecv_sem.at[way],
            device_id=peer(way),
            device_id_type=MESH,
        )

    def relay(way):
        gain_copy(way).wait_recv()
        gout[way] = (gmine[...] + gin[way].astype(f32)).astype(bf16)
        gain_copy(way).start()

    for way, goes, comes in ways:
        @pl.when(goes & jnp.logical_not(comes))
        def _():
            gout[way] = gmine[...].astype(bf16)
            gain_copy(way).start()

    launch(half, CHUNKS - 1)

    @pl.loop(half + 1, n - 1)
    def _(j):
        @pl.loop(0, CHUNKS)
        def _(c):
            step(j, c)

    near = (me < half, me >= half)
    tile_n = 640 if width % 640 == 0 else HEAD_DIM
    tiles_n = width // tile_n

    def forward(c):
        @pl.loop(0, tiles_n)
        def _(i):
            ns = pl.ds(pl.multiple_of(i * tile_n, tile_n), tile_n)
            value = jnp.dot(held[:, cols(c)], w[cols(c), ns], preferred_element_type=f32)
            if c == 0:
                acc[:, ns] = value
            else:
                acc[:, ns] += value

    first, second = CHUNKS // 4, CHUNKS - 1
    for c in range(CHUNKS):
        arrive(n - 1, c)
        prepare(n - 1, c)
        if c == first:
            for way, goes, comes in ways:
                @pl.when(near[way] & goes & comes)
                def _():
                    relay(way)
        if c != second:
            launch(n - 1, c)
        take(n - 1, c)
        forward(c)
    for way, goes, comes in ways:
        @pl.when(near[1 - way] & goes & comes)
        def _():
            relay(way)
    launch(n - 1, second)

    for h in range(heads):
        hs = slice(h * HEAD_DIM, (h + 1) * HEAD_DIM)
        x = acc[:, hs] * scale_ref[...] + bias[:, hs]
        turned = x * cos[...] + pltpu.roll(x, HEAD_DIM // 2, 1) * sin[...]
        plain = lax.rem(me * heads + h, GROUP) == GROUP - 1
        qkv[:, hs] = jnp.where(plain, x, turned).astype(bf16)

    loads[5].wait()
    scale = scale_ref[block(me), :][:, :1]
    inner = jnp.zeros((rows, 1), f32)
    for c in range(CHUNKS):
        ks = slice(c * span, (c + 1) * span)
        if c == CHUNKS - 1:
            for way, goes, comes in ways:
                @pl.when(comes & jnp.logical_not(goes))
                def _():
                    gain_copy(way).wait_recv()

                @pl.when(comes)
                def _():
                    gmine[...] += gin[way].astype(f32)
            for i in range(16):
                gg_ref[:, i * piece:(i + 1) * piece] = gmine[i:i + 1, :]
        tgp[:, ks] = part[block(me), ks]
        for way, goes, comes in ways:
            @pl.when(comes)
            def _():
                slot = me + 1 - way
                transfer(way, run, slot, n - 1, c).wait_recv()
                tgp[:, ks] += run[block(slot), ks].astype(f32)

        scaled = tgp[:, ks] * gain[:, ks]
        inner = inner + jnp.sum(scaled * tok[:, ks].astype(f32), axis=1, keepdims=True)
        tgp[:, ks] = scaled * scale

    weight[...] = jnp.broadcast_to(scale * scale * scale * (inner / depth), weight.shape)

    @pl.loop(0, n)
    def _(j):
        @pl.loop(0, CHUNKS)
        def _(c):
            for way, goes, comes in ways:
                @pl.when(goes)
                def _():
                    transfer(way, raw, 0, j, c).wait_send()

    for way, goes, comes in ways:
        @pl.when(goes)
        def _():
            gain_copy(way).wait_send()


def finish(qkv, tgp, tok, weight, gg, bg, qkv_h, tg_h, gg_h, bg_h, tg, sem):
    moves = ((qkv, qkv_h), (gg.at[0], gg_h), (bg.at[0], bg_h))
    copies = [pltpu.make_async_copy(src, dst, sem.at[i]) for i, (src, dst) in enumerate(moves)]
    for c in copies:
        c.start()
    factor = weight[:, :1]
    span = tg.shape[1] // PIECES
    for p in range(PIECES):
        ks = slice(p * span, (p + 1) * span)
        tg[:, ks] = tgp[:, ks] - tok[:, ks].astype(jnp.float32) * factor
        c = pltpu.make_async_copy(tg.at[:, ks], tg_h.at[:, ks], sem.at[3 + p])
        c.start()
        copies.append(c)
    for c in copies:
        c.wait()


def shards(n, tokens, norm_gain, qkv_weight, qkv_bias, qkv_grad):
    rows, depth = tokens.shape
    every, width = qkv_grad.shape
    cosine, sine = rope_tables(every, rows, SEQ_LEN // n)
    bf16, f32 = jnp.bfloat16, jnp.float32
    dma = pltpu.SemaphoreType.DMA
    hbm = pl.BlockSpec(memory_space=pl.ANY)
    vmem = pl.BlockSpec(memory_space=pltpu.VMEM)
    results = pl.pallas_call(
        functools.partial(kernel, n),
        out_shape=(
            pltpu.VMEM((every, width), bf16),
            pltpu.VMEM((rows, depth), f32),
            pltpu.VMEM((rows, depth), bf16),
            pltpu.VMEM((rows, HEAD_DIM), f32),
            pltpu.VMEM((1, depth), f32),
            pltpu.VMEM((1, width), f32),
        ),
        in_specs=[hbm] * 7,
        out_specs=[vmem] * 6,
        scratch_shapes=[
            pltpu.VMEM((every, depth), bf16),
            pltpu.VMEM((1, depth), f32),
            pltpu.VMEM((depth, width), bf16),
            pltpu.VMEM((1, width), f32),
            pltpu.VMEM((every, width), bf16),
            pltpu.VMEM((every, HEAD_DIM), f32),
            pltpu.VMEM((every, HEAD_DIM), f32),
            pltpu.VMEM((every, width), bf16),
            pltpu.VMEM((every, depth), f32),
            pltpu.VMEM((every, depth), bf16),
            pltpu.VMEM((every + rows, depth), bf16),
            pltpu.VMEM((every, width), f32),
            pltpu.VMEM((every, HEAD_DIM), f32),
            pltpu.VMEM((every, HEAD_DIM), f32),
            pltpu.VMEM((8, depth), f32),
            pltpu.VMEM((16, depth // 16), f32),
            pltpu.VMEM((2, 16, depth // 16), bf16),
            pltpu.VMEM((2, 16, depth // 16), bf16),
            dma((CHUNKS,)),
            dma((6,)),
            dma((depth // TILE_K,)),
            dma((2, n, CHUNKS)),
            dma((2, n, CHUNKS)),
            dma((2,)),
            dma((2,)),
            pltpu.SemaphoreType.REGULAR,
        ],
        compiler_params=pltpu.CompilerParams(
            collective_id=0, has_side_effects=True, vmem_limit_bytes=60000000
        ),
        cost_estimate=pl.CostEstimate(
            flops=4 * every * depth * width, bytes_accessed=2 * depth * width, transcendentals=0
        ),
    )(
        tokens, norm_gain, qkv_weight, qkv_bias, qkv_grad,
        jnp.asarray(cosine), jnp.asarray(sine),
    )
    return pl.pallas_call(
        finish,
        out_shape=(
            jax.ShapeDtypeStruct((every, width), bf16),
            jax.ShapeDtypeStruct((rows, depth), f32),
            jax.ShapeDtypeStruct((depth,), f32),
            jax.ShapeDtypeStruct((width,), f32),
        ),
        in_specs=[vmem] * 6,
        out_specs=[hbm] * 4,
        scratch_shapes=[pltpu.VMEM((rows, depth), f32), dma((3 + PIECES,))],
        compiler_params=pltpu.CompilerParams(vmem_limit_bytes=3 << 20),
    )(*results)


def solution(mesh):
    in_specs = (P(("dp", "mp"), None), P(), P(None, "mp"), P("mp"), P("dp", "mp"))
    out_specs = (P("dp", "mp"), P(("dp", "mp"), None), P("dp"), P(("dp", "mp")))
    body = functools.partial(shards, mesh.shape["mp"])
    return jax.shard_map(body, mesh=mesh, in_specs=in_specs, out_specs=out_specs, check_vma=False)
```

```python
import functools

import jax
import jax.numpy as jnp
import numpy as np
from jax import lax
from jax.experimental import pallas as pl
from jax.experimental.pallas import tpu as pltpu
from jax.sharding import PartitionSpec as P

HEAD_DIM = 128
SEQ_LEN = 32768
GROUP = 10
CHUNKS = 4
TILE_K = 512
PIECES = 4
DEPTH = 4
MESH = pl.DeviceIdType.MESH


def rope_tables(rows, tok_dev, stride):
    half = HEAD_DIM // 2
    row = np.arange(rows)
    place = (row // tok_dev * stride + row % tok_dev).astype(np.float32)
    inverse = np.exp(
        -np.log(np.float32(1000000.0))
        * (np.float32(2.0) * np.arange(half).astype(np.float32) / np.float32(HEAD_DIM))
    ).astype(np.float32)
    angle = (place[:, None] * inverse[None, :]).astype(np.float32)
    cosine, sine = np.cos(angle).astype(np.float32), np.sin(angle).astype(np.float32)
    return np.concatenate([cosine, cosine], 1), np.concatenate([-sine, sine], 1)


def kernel(
    n,
    tok_h, gain_h, w_h, bias_h, grad_h, turn_h,
    qkv, tgp, tok, weight, gg_ref, bg_ref,
    raw, gain, w, bias, grad, turn,
    low, part, held, run, acc, square, scale_ref, gsum, gmine, gout, gin,
    in_sem, w_sem, send_sem, recv_sem, gsend_sem, grecv_sem, ready,
):
    me = lax.axis_index("mp")
    rows, depth = tok.shape
    width = w.shape[1]
    heads = width // HEAD_DIM
    fold = 4 if heads % 4 == 0 else 1
    span = depth // CHUNKS
    tiles = depth // TILE_K
    per = tiles // CHUNKS
    half = n // 2
    f32, bf16 = jnp.float32, jnp.bfloat16
    every = low.shape[0]
    cos, sin = turn.at[:every], turn.at[every:]

    patient = lax.rem(lax.axis_index("dp"), 2) == 1
    has_right, has_left = me < n - 1, me > 0
    ways = ((0, has_right, has_left), (1, has_left, has_right))
    barrier = pltpu.get_barrier_semaphore()

    def peer(way):
        return {"mp": lax.rem(me + (1 if way == 0 else n - 1), n)}

    @pl.when(has_right)
    def _():
        pl.semaphore_signal(barrier, inc=1, device_id=peer(0), device_id_type=MESH)

    def block(s):
        return pl.ds(pl.multiple_of(s * rows, rows), rows)

    def cols(c):
        return pl.ds(pl.multiple_of(c * span, span), span)

    loads = []
    for i, (src, dst) in enumerate((
        (tok_h, raw.at[block(me), :]), (gain_h, gain.at[0]), (grad_h, grad),
        (turn_h, turn), (bias_h, bias.at[0]),
    )):
        loads.append(pltpu.make_async_copy(src, dst, in_sem.at[i]))

    def w_copy(i):
        k = pl.ds(pl.multiple_of(i * TILE_K, TILE_K), TILE_K)
        return pltpu.make_async_copy(w_h.at[k, :], w.at[k, :], w_sem.at[lax.rem(i, DEPTH)])

    def transfer(way, buf, at, j, c):
        ref = buf.at[block(at), cols(c)]
        return pltpu.make_async_remote_copy(
            src_ref=ref,
            dst_ref=ref,
            send_sem=send_sem.at[way, c],
            recv_sem=recv_sem.at[way, lax.rem(j, 2), c],
            device_id=peer(way),
            device_id_type=MESH,
        )

    def own(way, c):
        return pltpu.make_async_remote_copy(
            src_ref=tok_h.at[:, cols(c)],
            dst_ref=raw.at[block(me), cols(c)],
            send_sem=send_sem.at[way, c],
            recv_sem=recv_sem.at[way, 0, c],
            device_id=peer(way),
            device_id_type=MESH,
        )

    def absorb(b, c):
        v = raw[block(b), cols(c)].astype(f32)
        held[block(b), cols(c)] = (v * gain[:, cols(c)]).astype(bf16)
        v = v * v
        while v.shape[1] > HEAD_DIM:
            m = v.shape[1] // 2
            v = v[:, :m] + v[:, m:]
        if isinstance(c, int):
            old = jnp.zeros_like(v) if c == 0 else square[block(b), :]
        else:
            old = jnp.where(c == 0, jnp.zeros_like(v), square[block(b), :])
        square[block(b), :] = old + v

    def settle(b):
        total = jnp.sum(square[block(b), :], axis=1, keepdims=True)
        scale_ref[block(b), :] = jnp.broadcast_to(lax.rsqrt(total / depth + 1e-06), (rows, HEAD_DIM))

    def send(way):
        for c in range(CHUNKS):
            own(way, c).start()

    @pl.when(has_left)
    def _():
        pl.semaphore_wait(barrier, 1)
        pl.semaphore_signal(ready, inc=1, device_id=peer(1), device_id_type=MESH)
        send(1)

    for l in loads:
        l.start()

    @pl.loop(0, DEPTH)
    def _(i):
        w_copy(i).start()

    loads[0].wait()

    @pl.when(has_right)
    def _():
        pl.semaphore_wait(ready, 1)
        send(0)

    def arrive(j, c):
        for way, goes, comes in ways:
            @pl.when(comes)
            def _():
                transfer(way, raw, 0, j - 1, c).wait_recv()

    def prepare(j, c):
        for way, goes, comes in ways:
            back = me if way == 0 else n - 1 - me

            @pl.when(goes & (j > back))
            def _():
                t = n - j + me if way == 0 else j - n + me
                slot = t + 1 if way == 0 else t

                @pl.when(comes)
                def _():
                    value = part[block(t), cols(c)] + run[block(slot), cols(c)].astype(f32)
                    run[block(slot), cols(c)] = value.astype(bf16)

                @pl.when(jnp.logical_not(comes))
                def _():
                    run[block(slot), cols(c)] = part[block(t), cols(c)].astype(bf16)

    def launch(j, c):
        for way, goes, comes in ways:
            back = me if way == 0 else n - 1 - me

            @pl.when(goes)
            def _():
                transfer(way, raw, 0, 0, c).wait_send()

            @pl.when(goes & (j <= back))
            def _():
                transfer(way, raw, me - j if way == 0 else me + j, j, c).start()

            @pl.when(goes & (j > back))
            def _():
                t = n - j + me if way == 0 else j - n + me
                transfer(way, run, t + 1 if way == 0 else t, j, c).start()

    def take(j, c):
        for way, goes, comes in ways:
            back = me if way == 0 else n - 1 - me

            @pl.when(comes & (j <= back))
            def _():
                b = me - j if way == 0 else me + j
                absorb(b, c)
                if isinstance(c, int):
                    if c == CHUNKS - 1:
                        settle(b)
                else:
                    @pl.when(c == CHUNKS - 1)
                    def _():
                        settle(b)

    def step(j, c):
        arrive(j, c)
        prepare(j, c)
        launch(j, c)
        take(j, c)

    for l in loads[1:5]:
        l.wait()

    @pl.loop(0, heads // fold)
    def _(i):
        for p in range(fold):
            h = i * fold + p
            hs = pl.ds(pl.multiple_of(h * HEAD_DIM, HEAD_DIM), HEAD_DIM)
            x = grad[:, hs].astype(f32)
            turned = x * cos[...] - pltpu.roll(x, HEAD_DIM // 2, 1) * sin[...]
            plain = lax.rem(me * heads + h, GROUP) == GROUP - 1
            x = jnp.where(plain, x, turned)
            bg_ref[:, hs] = jnp.sum(x, axis=0, keepdims=True)
            low[:, hs] = x.astype(bf16)

    def backward(c):
        @pl.loop(0, per)
        def _(i):
            at = c * per + i
            w_copy(at).wait()

            @pl.when(at + DEPTH < tiles)
            def _():
                w_copy(at + DEPTH).start()

            k = pl.ds(pl.multiple_of(at * TILE_K, TILE_K), TILE_K)
            part[:, k] = lax.dot_general(
                low[...], w[k, :], (((1,), (1,)), ((), ())), preferred_element_type=f32
            )

    @pl.loop(0, CHUNKS)
    def _(c):
        backward(c)
        step(1, c)

    @pl.loop(0, CHUNKS)
    def _(c):
        absorb(me, c)
        tok[:, cols(c)] = raw[block(me), cols(c)]

    settle(me)

    @pl.loop(2, half)
    def _(j):
        @pl.loop(0, CHUNKS)
        def _(c):
            step(j, c)

    @pl.loop(0, CHUNKS)
    def _(c):
        arrive(half, c)
        prepare(half, c)

        @pl.when(c < CHUNKS - 1)
        def _():
            launch(half, c)

        take(half, c)


    def gain_add(source, at, t):
        scale = scale_ref[block(t), :]

        @pl.loop(0, depth // 1024)
        def _(i):
            for p in range(1024 // HEAD_DIM):
                k = pl.ds(pl.multiple_of(i * 1024 + p * HEAD_DIM, HEAD_DIM), HEAD_DIM)
                x = source[block(at), k].astype(f32) * raw[block(t), k].astype(f32) * scale
                total = x[:8]
                for r in range(8, rows, 8):
                    total = total + x[r:r + 8]
                gsum[:, k] += total

    gsum[...] = jnp.zeros_like(gsum)

    @pl.loop(0, n)
    def _(t):
        @pl.when((me - t < half) & (t - me < half))
        def _():
            gain_add(part, t, t)

    @pl.when(me >= half)
    def _():
        gain_add(run, me - half, me - half)

    @pl.when(me + half < n)
    def _():
        gain_add(run, me + half + 1, me + half)

    piece = depth // 16
    for i in range(16):
        gmine[i:i + 1, :] = jnp.sum(gsum[:, i * piece:(i + 1) * piece], axis=0, keepdims=True)

    def gain_copy(way):
        return pltpu.make_async_remote_copy(
            src_ref=gout.at[way],
            dst_ref=gin.at[way],
            send_sem=gsend_sem.at[way],
            recv_sem=grecv_sem.at[way],
            device_id=peer(way),
            device_id_type=MESH,
        )

    def relay(way):
        gain_copy(way).wait_recv()
        gout[way] = (gmine[...] + gin[way].astype(f32)).astype(bf16)
        gain_copy(way).start()

    for way, goes, comes in ways:
        @pl.when(goes & jnp.logical_not(comes))
        def _():
            gout[way] = gmine[...].astype(bf16)
            gain_copy(way).start()

    launch(half, CHUNKS - 1)

    @pl.loop(half + 1, n - 1)
    def _(j):
        @pl.loop(0, CHUNKS)
        def _(c):
            step(j, c)

    near = (me < half, me >= half)
    tile_n = 640 if width % 640 == 0 else HEAD_DIM
    tiles_n = width // tile_n

    def forward(c):
        @pl.loop(0, tiles_n)
        def _(i):
            ns = pl.ds(pl.multiple_of(i * tile_n, tile_n), tile_n)
            value = jnp.dot(held[:, cols(c)], w[cols(c), ns], preferred_element_type=f32)

            @pl.when(c == 0)
            def _():
                acc[:, ns] = value

            @pl.when(c > 0)
            def _():
                acc[:, ns] += value

    first, second = CHUNKS // 4, CHUNKS - 1
    @pl.loop(0, CHUNKS)
    def _(c):
        arrive(n - 1, c)
        prepare(n - 1, c)
        for way, goes, comes in ways:
            @pl.when(
                goes & comes & ((near[way] & (c == first)) | (near[1 - way] & (c == second)))
            )
            def _():
                relay(way)

        @pl.when(jnp.logical_not(patient & (c == CHUNKS - 1)))
        def _():
            launch(n - 1, c)

        take(n - 1, c)
        forward(c)

    @pl.loop(0, heads // fold)
    def _(i):
        for p in range(fold):
            h = i * fold + p
            hs = pl.ds(pl.multiple_of(h * HEAD_DIM, HEAD_DIM), HEAD_DIM)
            x = acc[:, hs] * scale_ref[...] + bias[:, hs]
            turned = x * cos[...] + pltpu.roll(x, HEAD_DIM // 2, 1) * sin[...]
            plain = lax.rem(me * heads + h, GROUP) == GROUP - 1
            qkv[:, hs] = jnp.where(plain, x, turned).astype(bf16)

    scale = scale_ref[block(me), :][:, :1]
    inner = jnp.zeros((rows, 1), f32)
    for c in range(CHUNKS):
        ks = slice(c * span, (c + 1) * span)
        if c == CHUNKS - 2:
            @pl.when(patient)
            def _():
                pl.delay(1000)
                launch(n - 1, CHUNKS - 1)

        if c == CHUNKS - 1:
            for way, goes, comes in ways:
                @pl.when(comes & jnp.logical_not(goes))
                def _():
                    gain_copy(way).wait_recv()

                @pl.when(comes)
                def _():
                    gmine[...] += gin[way].astype(f32)
            for i in range(16):
                gg_ref[:, i * piece:(i + 1) * piece] = gmine[i:i + 1, :]
        tgp[:, ks] = part[block(me), ks]
        for way, goes, comes in ways:
            @pl.when(comes)
            def _():
                slot = me + 1 - way
                transfer(way, run, slot, n - 1, c).wait_recv()
                tgp[:, ks] += run[block(slot), ks].astype(f32)

        scaled = tgp[:, ks] * gain[:, ks]
        inner = inner + jnp.sum(scaled * tok[:, ks].astype(f32), axis=1, keepdims=True)
        tgp[:, ks] = scaled * scale

    weight[...] = jnp.broadcast_to(scale * scale * scale * (inner / depth), weight.shape)

    for way, goes, comes in ways:
        @pl.when(goes)
        def _():
            gain_copy(way).wait_send()
            for c in range(CHUNKS):
                transfer(way, raw, 0, 0, c).wait_send()


def finish(qkv, tgp, tok, weight, gg, bg, qkv_h, tg_h, gg_h, bg_h, tg, sem):
    moves = ((qkv, qkv_h), (gg.at[0], gg_h), (bg.at[0], bg_h))
    copies = [pltpu.make_async_copy(src, dst, sem.at[i]) for i, (src, dst) in enumerate(moves)]
    for c in copies:
        c.start()
    factor = weight[:, :1]
    span = tg.shape[1] // PIECES
    for p in range(PIECES):
        ks = slice(p * span, (p + 1) * span)
        tg[:, ks] = tgp[:, ks] - tok[:, ks].astype(jnp.float32) * factor
        c = pltpu.make_async_copy(tg.at[:, ks], tg_h.at[:, ks], sem.at[3 + p])
        c.start()
        copies.append(c)
    for c in copies:
        c.wait()


def shards(n, tokens, norm_gain, qkv_weight, qkv_bias, qkv_grad):
    rows, depth = tokens.shape
    every, width = qkv_grad.shape
    cosine, sine = rope_tables(every, rows, SEQ_LEN // n)
    bf16, f32 = jnp.bfloat16, jnp.float32
    dma = pltpu.SemaphoreType.DMA
    hbm = pl.BlockSpec(memory_space=pl.ANY)
    vmem = pl.BlockSpec(memory_space=pltpu.VMEM)
    results = pl.pallas_call(
        functools.partial(kernel, n),
        out_shape=(
            pltpu.VMEM((every, width), bf16),
            pltpu.VMEM((rows, depth), f32),
            pltpu.VMEM((rows, depth), bf16),
            pltpu.VMEM((rows, HEAD_DIM), f32),
            pltpu.VMEM((1, depth), f32),
            pltpu.VMEM((1, width), f32),
        ),
        in_specs=[hbm] * 6,
        out_specs=[vmem] * 6,
        scratch_shapes=[
            pltpu.VMEM((every, depth), bf16),
            pltpu.VMEM((1, depth), f32),
            pltpu.VMEM((depth, width), bf16),
            pltpu.VMEM((1, width), f32),
            pltpu.VMEM((every, width), bf16),
            pltpu.VMEM((2 * every, HEAD_DIM), f32),
            pltpu.VMEM((every, width), bf16),
            pltpu.VMEM((every, depth), f32),
            pltpu.VMEM((every, depth), bf16),
            pltpu.VMEM((every + rows, depth), bf16),
            pltpu.VMEM((every, width), f32),
            pltpu.VMEM((every, HEAD_DIM), f32),
            pltpu.VMEM((every, HEAD_DIM), f32),
            pltpu.VMEM((8, depth), f32),
            pltpu.VMEM((16, depth // 16), f32),
            pltpu.VMEM((2, 16, depth // 16), bf16),
            pltpu.VMEM((2, 16, depth // 16), bf16),
            dma((5,)),
            dma((DEPTH,)),
            dma((2, CHUNKS)),
            dma((2, 2, CHUNKS)),
            dma((2,)),
            dma((2,)),
            pltpu.SemaphoreType.REGULAR,
        ],
        compiler_params=pltpu.CompilerParams(
            collective_id=0, has_side_effects=True, vmem_limit_bytes=60000000
        ),
        cost_estimate=pl.CostEstimate(
            flops=4 * every * depth * width, bytes_accessed=2 * depth * width, transcendentals=0
        ),
    )(
        tokens, norm_gain, qkv_weight, qkv_bias, qkv_grad,
        jnp.asarray(np.concatenate([cosine, sine])),
    )
    return pl.pallas_call(
        finish,
        out_shape=(
            jax.ShapeDtypeStruct((every, width), bf16),
            jax.ShapeDtypeStruct((rows, depth), f32),
            jax.ShapeDtypeStruct((depth,), f32),
            jax.ShapeDtypeStruct((width,), f32),
        ),
        in_specs=[vmem] * 6,
        out_specs=[hbm] * 4,
        scratch_shapes=[pltpu.VMEM((rows, depth), f32), dma((3 + PIECES,))],
        compiler_params=pltpu.CompilerParams(vmem_limit_bytes=3 << 20),
    )(*results)


def solution(mesh):
    in_specs = (P(("dp", "mp"), None), P(), P(None, "mp"), P("mp"), P("dp", "mp"))
    out_specs = (P("dp", "mp"), P(("dp", "mp"), None), P("dp"), P(("dp", "mp")))
    body = functools.partial(shards, mesh.shape["mp"])
    return jax.shard_map(body, mesh=mesh, in_specs=in_specs, out_specs=out_specs, check_vma=False)
```

```python
import functools

import jax
import jax.numpy as jnp
import numpy as np
from jax import lax
from jax.experimental import pallas as pl
from jax.experimental.pallas import tpu as pltpu
from jax.sharding import PartitionSpec as P

HEAD_DIM = 128
SEQ_LEN = 32768
GROUP = 10
CHUNKS = 4
TILE_K = 512
PIECES = 2
DELAY = 1600
DEPTH = 4
MESH = pl.DeviceIdType.MESH


def rope_tables(rows, tok_dev, stride):
    half = HEAD_DIM // 2
    row = np.arange(rows)
    place = (row // tok_dev * stride + row % tok_dev).astype(np.float32)
    inverse = np.exp(
        -np.log(np.float32(1000000.0))
        * (np.float32(2.0) * np.arange(half).astype(np.float32) / np.float32(HEAD_DIM))
    ).astype(np.float32)
    angle = (place[:, None] * inverse[None, :]).astype(np.float32)
    cosine, sine = np.cos(angle).astype(np.float32), np.sin(angle).astype(np.float32)
    return np.concatenate([cosine, cosine], 1), np.concatenate([-sine, sine], 1)


def kernel(
    n,
    tok_h, gain_h, w_h, bias_h, grad_h, turn_h,
    qkv, tgp, tok, weight, gg_ref, bg_ref,
    raw, gain, w, bias, grad, turn,
    low, part, held, run, acc, square, scale_ref, gsum, gmine, gout, gin, sums,
    in_sem, w_sem, send_sem, recv_sem, gsend_sem, grecv_sem, ready,
):
    me = lax.axis_index("mp")
    rows, depth = tok.shape
    width = w.shape[1]
    heads = width // HEAD_DIM
    fold = 4 if heads % 4 == 0 else 1
    span = depth // CHUNKS
    tiles = depth // TILE_K
    per = tiles // CHUNKS
    half = n // 2
    f32, bf16 = jnp.float32, jnp.bfloat16
    every = low.shape[0]
    cos, sin = turn.at[:every], turn.at[every:]

    patient = lax.rem(lax.axis_index("dp"), 2) == 1
    has_right, has_left = me < n - 1, me > 0
    ways = ((0, has_right, has_left), (1, has_left, has_right))
    barrier = pltpu.get_barrier_semaphore()

    def peer(way):
        return {"mp": lax.rem(me + (1 if way == 0 else n - 1), n)}

    @pl.when(has_right)
    def _():
        pl.semaphore_signal(barrier, inc=1, device_id=peer(0), device_id_type=MESH)

    def block(s):
        return pl.ds(pl.multiple_of(s * rows, rows), rows)

    def cols(c):
        return pl.ds(pl.multiple_of(c * span, span), span)

    loads = []
    for i, (src, dst) in enumerate((
        (tok_h, raw.at[block(me), :]), (gain_h, gain.at[0]), (grad_h, grad),
        (turn_h, turn), (bias_h, bias.at[0]),
    )):
        loads.append(pltpu.make_async_copy(src, dst, in_sem.at[i]))

    def w_copy(i):
        k = pl.ds(pl.multiple_of(i * TILE_K, TILE_K), TILE_K)
        return pltpu.make_async_copy(w_h.at[k, :], w.at[k, :], w_sem.at[lax.rem(i, DEPTH)])

    def transfer(way, buf, at, j, c):
        ref = buf.at[block(at), cols(c)]
        return pltpu.make_async_remote_copy(
            src_ref=ref,
            dst_ref=ref,
            send_sem=send_sem.at[way, lax.rem(j, 2)],
            recv_sem=recv_sem.at[way, lax.rem(j, 2), c],
            device_id=peer(way),
            device_id_type=MESH,
        )

    def drain(way, j):
        ref = raw.at[block(0), :]
        pltpu.make_async_remote_copy(
            src_ref=ref,
            dst_ref=ref,
            send_sem=send_sem.at[way, lax.rem(j, 2)],
            recv_sem=recv_sem.at[way, 0, 0],
            device_id=peer(way),
            device_id_type=MESH,
        ).wait_send()

    def own(way, c):
        return pltpu.make_async_remote_copy(
            src_ref=tok_h.at[:, cols(c)],
            dst_ref=raw.at[block(me), cols(c)],
            send_sem=send_sem.at[way, 0],
            recv_sem=recv_sem.at[way, 0, c],
            device_id=peer(way),
            device_id_type=MESH,
        )

    def lanes(v):
        while v.shape[1] > HEAD_DIM:
            m = v.shape[1] // 2
            v = v[:, :m] + v[:, m:]
        return v

    def absorb(b, c):
        v = raw[block(b), cols(c)].astype(f32)
        held[block(b), cols(c)] = (v * gain[:, cols(c)]).astype(bf16)
        v = lanes(v * v)
        if isinstance(c, int):
            old = jnp.zeros_like(v) if c == 0 else square[block(b), :]
        else:
            old = jnp.where(c == 0, jnp.zeros_like(v), square[block(b), :])
        square[block(b), :] = old + v

    def settle(b):
        total = jnp.sum(square[block(b), :], axis=1, keepdims=True)
        scale_ref[block(b), :] = jnp.broadcast_to(lax.rsqrt(total / depth + 1e-06), (rows, HEAD_DIM))

    def send(way):
        for c in range(CHUNKS):
            own(way, c).start()

    @pl.when(has_left)
    def _():
        pl.semaphore_wait(barrier, 1)
        pl.semaphore_signal(ready, inc=1, device_id=peer(1), device_id_type=MESH)
        send(1)

    for l in loads:
        l.start()

    @pl.loop(0, DEPTH)
    def _(i):
        w_copy(i).start()

    loads[0].wait()

    @pl.when(has_right)
    def _():
        pl.semaphore_wait(ready, 1)
        send(0)

    def arrive(j, c):
        for way, goes, comes in ways:
            @pl.when(comes)
            def _():
                transfer(way, raw, 0, j - 1, c).wait_recv()

    def prepare(j, c):
        for way, goes, comes in ways:
            back = me if way == 0 else n - 1 - me

            @pl.when(goes & (j > back))
            def _():
                t = n - j + me if way == 0 else j - n + me
                slot = t + 1 if way == 0 else t

                @pl.when(comes)
                def _():
                    value = part[block(t), cols(c)] + run[block(slot), cols(c)].astype(f32)
                    run[block(slot), cols(c)] = value.astype(bf16)

                @pl.when(jnp.logical_not(comes))
                def _():
                    run[block(slot), cols(c)] = part[block(t), cols(c)].astype(bf16)

    def launch(j, c):
        for way, goes, comes in ways:
            back = me if way == 0 else n - 1 - me

            if not isinstance(j, int) or j >= 2:
                @pl.when(goes & (c == 0))
                def _():
                    drain(way, j)

            @pl.when(goes & (j <= back))
            def _():
                transfer(way, raw, me - j if way == 0 else me + j, j, c).start()

            @pl.when(goes & (j > back))
            def _():
                t = n - j + me if way == 0 else j - n + me
                transfer(way, run, t + 1 if way == 0 else t, j, c).start()

    def take(j, c):
        for way, goes, comes in ways:
            back = me if way == 0 else n - 1 - me

            @pl.when(comes & (j <= back))
            def _():
                b = me - j if way == 0 else me + j
                absorb(b, c)
                if isinstance(c, int):
                    if c == CHUNKS - 1:
                        settle(b)
                else:
                    @pl.when(c == CHUNKS - 1)
                    def _():
                        settle(b)

    def step(j, c):
        arrive(j, c)
        prepare(j, c)
        launch(j, c)
        take(j, c)

    for l in loads[1:5]:
        l.wait()

    @pl.loop(0, heads // fold)
    def _(i):
        for p in range(fold):
            h = i * fold + p
            hs = pl.ds(pl.multiple_of(h * HEAD_DIM, HEAD_DIM), HEAD_DIM)
            x = grad[:, hs].astype(f32)
            turned = x * cos[...] - pltpu.roll(x, HEAD_DIM // 2, 1) * sin[...]
            plain = lax.rem(me * heads + h, GROUP) == GROUP - 1
            x = jnp.where(plain, x, turned)
            bg_ref[:, hs] = jnp.sum(x, axis=0, keepdims=True)
            low[:, hs] = x.astype(bf16)

    def backward(c):
        @pl.loop(0, per)
        def _(i):
            at = c * per + i
            w_copy(at).wait()

            @pl.when(at + DEPTH < tiles)
            def _():
                w_copy(at + DEPTH).start()

            k = pl.ds(pl.multiple_of(at * TILE_K, TILE_K), TILE_K)
            part[:, k] = lax.dot_general(
                low[...], w[k, :], (((1,), (1,)), ((), ())), preferred_element_type=f32
            )

    @pl.loop(0, CHUNKS)
    def _(c):
        backward(c)
        step(1, c)

    @pl.loop(0, CHUNKS)
    def _(c):
        absorb(me, c)
        tok[:, cols(c)] = raw[block(me), cols(c)]

    settle(me)

    @pl.loop(2, half)
    def _(j):
        @pl.loop(0, CHUNKS)
        def _(c):
            step(j, c)

    @pl.loop(0, CHUNKS)
    def _(c):
        arrive(half, c)
        prepare(half, c)

        @pl.when(c < CHUNKS - 1)
        def _():
            launch(half, c)

        take(half, c)


    def gain_add(source, at, t):
        scale = scale_ref[block(t), :]

        @pl.loop(0, depth // 1024)
        def _(i):
            for p in range(1024 // HEAD_DIM):
                k = pl.ds(pl.multiple_of(i * 1024 + p * HEAD_DIM, HEAD_DIM), HEAD_DIM)
                x = source[block(at), k].astype(f32) * raw[block(t), k].astype(f32) * scale
                total = x[:8]
                for r in range(8, rows, 8):
                    total = total + x[r:r + 8]
                gsum[:, k] += total

    gsum[...] = jnp.zeros_like(gsum)

    @pl.loop(0, n)
    def _(t):
        @pl.when((me - t < half) & (t - me < half))
        def _():
            gain_add(part, t, t)

    @pl.when(me >= half)
    def _():
        gain_add(run, me - half, me - half)

    @pl.when(me + half < n)
    def _():
        gain_add(run, me + half + 1, me + half)

    piece = depth // 16
    for i in range(16):
        gmine[i:i + 1, :] = jnp.sum(gsum[:, i * piece:(i + 1) * piece], axis=0, keepdims=True)

    def gain_copy(way):
        return pltpu.make_async_remote_copy(
            src_ref=gout.at[way],
            dst_ref=gin.at[way],
            send_sem=gsend_sem.at[way],
            recv_sem=grecv_sem.at[way],
            device_id=peer(way),
            device_id_type=MESH,
        )

    def relay(way):
        gain_copy(way).wait_recv()
        gout[way] = (gmine[...] + gin[way].astype(f32)).astype(bf16)
        gain_copy(way).start()

    for way, goes, comes in ways:
        @pl.when(goes & jnp.logical_not(comes))
        def _():
            gout[way] = gmine[...].astype(bf16)
            gain_copy(way).start()

    launch(half, CHUNKS - 1)

    @pl.loop(half + 1, n - 1)
    def _(j):
        @pl.loop(0, CHUNKS)
        def _(c):
            step(j, c)

    near = (me < half, me >= half)
    tile_n = 640 if width % 640 == 0 else HEAD_DIM
    tiles_n = width // tile_n

    def forward(c):
        @pl.loop(0, tiles_n)
        def _(i):
            ns = pl.ds(pl.multiple_of(i * tile_n, tile_n), tile_n)
            value = jnp.dot(held[:, cols(c)], w[cols(c), ns], preferred_element_type=f32)

            @pl.when(c == 0)
            def _():
                acc[:, ns] = value

            @pl.when(c > 0)
            def _():
                acc[:, ns] += value

    first, second = CHUNKS // 4, CHUNKS - 1
    @pl.loop(0, CHUNKS)
    def _(c):
        arrive(n - 1, c)
        prepare(n - 1, c)
        for way, goes, comes in ways:
            @pl.when(
                goes & comes & ((near[way] & (c == first)) | (near[1 - way] & (c == second)))
            )
            def _():
                relay(way)

        @pl.when(jnp.logical_not(patient & (c == CHUNKS - 1)))
        def _():
            launch(n - 1, c)

        take(n - 1, c)
        forward(c)

    @pl.loop(0, heads // fold)
    def _(i):
        for p in range(fold):
            h = i * fold + p
            hs = pl.ds(pl.multiple_of(h * HEAD_DIM, HEAD_DIM), HEAD_DIM)
            x = acc[:, hs] * scale_ref[...] + bias[:, hs]
            turned = x * cos[...] + pltpu.roll(x, HEAD_DIM // 2, 1) * sin[...]
            plain = lax.rem(me * heads + h, GROUP) == GROUP - 1
            qkv[:, hs] = jnp.where(plain, x, turned).astype(bf16)

    scale = scale_ref[block(me), :][:, :1]
    sums[...] = jnp.zeros_like(sums)

    def close(ks, slots):
        value = part[block(me), ks]
        for slot in slots:
            value = value + run[block(slot), ks].astype(f32)
        value = value * gain[:, ks]
        tgp[:, ks] = value * scale
        sums[...] += lanes(value * tok[:, ks].astype(f32))

    for c in range(CHUNKS):
        ks = slice(c * span, (c + 1) * span)
        if c == CHUNKS - 2:
            @pl.when(patient)
            def _():
                pl.delay(DELAY)
                launch(n - 1, CHUNKS - 1)

        if c == CHUNKS - 1:
            for way, goes, comes in ways:
                @pl.when(comes & jnp.logical_not(goes))
                def _():
                    gain_copy(way).wait_recv()

                @pl.when(comes)
                def _():
                    gmine[...] += gin[way].astype(f32)
            for i in range(16):
                gg_ref[:, i * piece:(i + 1) * piece] = gmine[i:i + 1, :]
        for way, goes, comes in ways:
            @pl.when(comes)
            def _():
                transfer(way, run, me + 1 - way, n - 1, c).wait_recv()

        @pl.when(has_left & has_right)
        def _():
            close(ks, (me + 1, me))

        @pl.when(jnp.logical_not(has_right))
        def _():
            close(ks, (me + 1,))

        @pl.when(jnp.logical_not(has_left))
        def _():
            close(ks, (me,))

    inner = jnp.sum(sums[...], axis=1, keepdims=True)
    weight[...] = jnp.broadcast_to(scale * scale * scale * (inner / depth), weight.shape)

    for way, goes, comes in ways:
        @pl.when(goes)
        def _():
            gain_copy(way).wait_send()
            drain(way, n - 2)
            drain(way, n - 1)


def finish(qkv, tgp, tok, weight, gg, bg, qkv_h, tg_h, gg_h, bg_h, tg, sem):
    moves = ((qkv, qkv_h), (gg.at[0], gg_h), (bg.at[0], bg_h))
    copies = [pltpu.make_async_copy(src, dst, sem.at[i]) for i, (src, dst) in enumerate(moves)]
    for c in copies:
        c.start()
    factor = weight[:, :1]
    span = tg.shape[1] // PIECES
    for p in range(PIECES):
        ks = slice(p * span, (p + 1) * span)
        tg[:, ks] = tgp[:, ks] - tok[:, ks].astype(jnp.float32) * factor
        c = pltpu.make_async_copy(tg.at[:, ks], tg_h.at[:, ks], sem.at[3 + p])
        c.start()
        copies.append(c)
    for c in copies:
        c.wait()


def shards(n, tokens, norm_gain, qkv_weight, qkv_bias, qkv_grad):
    rows, depth = tokens.shape
    every, width = qkv_grad.shape
    cosine, sine = rope_tables(every, rows, SEQ_LEN // n)
    bf16, f32 = jnp.bfloat16, jnp.float32
    dma = pltpu.SemaphoreType.DMA
    hbm = pl.BlockSpec(memory_space=pl.ANY)
    vmem = pl.BlockSpec(memory_space=pltpu.VMEM)
    results = pl.pallas_call(
        functools.partial(kernel, n),
        out_shape=(
            pltpu.VMEM((every, width), bf16),
            pltpu.VMEM((rows, depth), f32),
            pltpu.VMEM((rows, depth), bf16),
            pltpu.VMEM((rows, HEAD_DIM), f32),
            pltpu.VMEM((1, depth), f32),
            pltpu.VMEM((1, width), f32),
        ),
        in_specs=[hbm] * 6,
        out_specs=[vmem] * 6,
        scratch_shapes=[
            pltpu.VMEM((every, depth), bf16),
            pltpu.VMEM((1, depth), f32),
            pltpu.VMEM((depth, width), bf16),
            pltpu.VMEM((1, width), f32),
            pltpu.VMEM((every, width), bf16),
            pltpu.VMEM((2 * every, HEAD_DIM), f32),
            pltpu.VMEM((every, width), bf16),
            pltpu.VMEM((every, depth), f32),
            pltpu.VMEM((every, depth), bf16),
            pltpu.VMEM((every + rows, depth), bf16),
            pltpu.VMEM((every, width), f32),
            pltpu.VMEM((every, HEAD_DIM), f32),
            pltpu.VMEM((every, HEAD_DIM), f32),
            pltpu.VMEM((8, depth), f32),
            pltpu.VMEM((16, depth // 16), f32),
            pltpu.VMEM((2, 16, depth // 16), bf16),
            pltpu.VMEM((2, 16, depth // 16), bf16),
            pltpu.VMEM((rows, HEAD_DIM), f32),
            dma((5,)),
            dma((DEPTH,)),
            dma((2, 2)),
            dma((2, 2, CHUNKS)),
            dma((2,)),
            dma((2,)),
            pltpu.SemaphoreType.REGULAR,
        ],
        compiler_params=pltpu.CompilerParams(
            collective_id=0, has_side_effects=True, vmem_limit_bytes=60000000
        ),
        cost_estimate=pl.CostEstimate(
            flops=4 * every * depth * width, bytes_accessed=2 * depth * width, transcendentals=0
        ),
    )(
        tokens, norm_gain, qkv_weight, qkv_bias, qkv_grad,
        jnp.asarray(np.concatenate([cosine, sine])),
    )
    return pl.pallas_call(
        finish,
        out_shape=(
            jax.ShapeDtypeStruct((every, width), bf16),
            jax.ShapeDtypeStruct((rows, depth), f32),
            jax.ShapeDtypeStruct((depth,), f32),
            jax.ShapeDtypeStruct((width,), f32),
        ),
        in_specs=[vmem] * 6,
        out_specs=[hbm] * 4,
        scratch_shapes=[pltpu.VMEM((rows, depth), f32), dma((3 + PIECES,))],
        compiler_params=pltpu.CompilerParams(vmem_limit_bytes=3 << 20),
    )(*results)


def solution(mesh):
    in_specs = (P(("dp", "mp"), None), P(), P(None, "mp"), P("mp"), P("dp", "mp"))
    out_specs = (P("dp", "mp"), P(("dp", "mp"), None), P("dp"), P(("dp", "mp")))
    body = functools.partial(shards, mesh.shape["mp"])
    return jax.shard_map(body, mesh=mesh, in_specs=in_specs, out_specs=out_specs, check_vma=False)
```

```python
import functools

import jax
import jax.numpy as jnp
import numpy as np
from jax import lax
from jax.experimental import pallas as pl
from jax.experimental.pallas import tpu as pltpu
from jax.sharding import PartitionSpec as P

HEAD_DIM = 128
SEQ_LEN = 32768
GROUP = 10
CHUNKS = 4
TILE_K = 512
PIECES = 2
DEPTH = 4
MESH = pl.DeviceIdType.MESH


def rope_tables(rows, tok_dev, stride):
    half = HEAD_DIM // 2
    row = np.arange(rows)
    place = (row // tok_dev * stride + row % tok_dev).astype(np.float32)
    inverse = np.exp(
        -np.log(np.float32(1000000.0))
        * (np.float32(2.0) * np.arange(half).astype(np.float32) / np.float32(HEAD_DIM))
    ).astype(np.float32)
    angle = (place[:, None] * inverse[None, :]).astype(np.float32)
    cosine, sine = np.cos(angle).astype(np.float32), np.sin(angle).astype(np.float32)
    return np.concatenate([cosine, cosine], 1), np.concatenate([-sine, sine], 1)


def kernel(
    n,
    tok_h, gain_h, w_h, bias_h, grad_h, turn_h,
    qkv, tgp, tok, weight, gg_ref, bg_ref,
    raw, gain, w, bias, grad, turn,
    low, part, held, run, acc, square, scale_ref, gsum, gmine, gout, gin,
    in_sem, w_sem, send_sem, recv_sem, gsend_sem, grecv_sem, ready,
):
    me = lax.axis_index("mp")
    rows, depth = tok.shape
    width = w.shape[1]
    heads = width // HEAD_DIM
    fold = 4 if heads % 4 == 0 else 1
    span = depth // CHUNKS
    tiles = depth // TILE_K
    per = tiles // CHUNKS
    half = n // 2
    f32, bf16 = jnp.float32, jnp.bfloat16
    every = low.shape[0]
    cos, sin = turn.at[:every], turn.at[every:]

    patient = lax.rem(lax.axis_index("dp"), 2) == 1
    has_right, has_left = me < n - 1, me > 0
    ways = ((0, has_right, has_left), (1, has_left, has_right))
    barrier = pltpu.get_barrier_semaphore()

    def peer(way):
        return {"mp": lax.rem(me + (1 if way == 0 else n - 1), n)}

    @pl.when(has_right)
    def _():
        pl.semaphore_signal(barrier, inc=1, device_id=peer(0), device_id_type=MESH)

    def block(s):
        return pl.ds(pl.multiple_of(s * rows, rows), rows)

    def cols(c):
        return pl.ds(pl.multiple_of(c * span, span), span)

    loads = []
    for i, (src, dst) in enumerate((
        (tok_h, raw.at[block(me), :]), (gain_h, gain.at[0]), (grad_h, grad),
        (turn_h, turn), (bias_h, bias.at[0]),
    )):
        loads.append(pltpu.make_async_copy(src, dst, in_sem.at[i]))

    def w_copy(i):
        k = pl.ds(pl.multiple_of(i * TILE_K, TILE_K), TILE_K)
        return pltpu.make_async_copy(w_h.at[k, :], w.at[k, :], w_sem.at[lax.rem(i, DEPTH)])

    def transfer(way, buf, at, j, c):
        ref = buf.at[block(at), cols(c)]
        return pltpu.make_async_remote_copy(
            src_ref=ref,
            dst_ref=ref,
            send_sem=send_sem.at[way, c],
            recv_sem=recv_sem.at[way, lax.rem(j, 2), c],
            device_id=peer(way),
            device_id_type=MESH,
        )

    def own(way, c):
        return pltpu.make_async_remote_copy(
            src_ref=tok_h.at[:, cols(c)],
            dst_ref=raw.at[block(me), cols(c)],
            send_sem=send_sem.at[way, c],
            recv_sem=recv_sem.at[way, 0, c],
            device_id=peer(way),
            device_id_type=MESH,
        )

    def absorb(b, c):
        v = raw[block(b), cols(c)].astype(f32)
        held[block(b), cols(c)] = (v * gain[:, cols(c)]).astype(bf16)
        v = v * v
        while v.shape[1] > HEAD_DIM:
            m = v.shape[1] // 2
            v = v[:, :m] + v[:, m:]
        if isinstance(c, int):
            old = jnp.zeros_like(v) if c == 0 else square[block(b), :]
        else:
            old = jnp.where(c == 0, jnp.zeros_like(v), square[block(b), :])
        square[block(b), :] = old + v

    def settle(b):
        total = jnp.sum(square[block(b), :], axis=1, keepdims=True)
        scale_ref[block(b), :] = jnp.broadcast_to(lax.rsqrt(total / depth + 1e-06), (rows, HEAD_DIM))

    def send(way):
        for c in range(CHUNKS):
            own(way, c).start()

    @pl.when(has_left)
    def _():
        pl.semaphore_wait(barrier, 1)
        pl.semaphore_signal(ready, inc=1, device_id=peer(1), device_id_type=MESH)
        send(1)

    for l in loads:
        l.start()

    @pl.loop(0, DEPTH)
    def _(i):
        w_copy(i).start()

    loads[0].wait()

    @pl.when(has_right)
    def _():
        pl.semaphore_wait(ready, 1)
        send(0)

    def arrive(j, c):
        for way, goes, comes in ways:
            @pl.when(comes)
            def _():
                transfer(way, raw, 0, j - 1, c).wait_recv()

    def prepare(j, c):
        for way, goes, comes in ways:
            back = me if way == 0 else n - 1 - me

            @pl.when(goes & (j > back))
            def _():
                t = n - j + me if way == 0 else j - n + me
                slot = t + 1 if way == 0 else t

                @pl.when(comes)
                def _():
                    value = part[block(t), cols(c)] + run[block(slot), cols(c)].astype(f32)
                    run[block(slot), cols(c)] = value.astype(bf16)

                @pl.when(jnp.logical_not(comes))
                def _():
                    run[block(slot), cols(c)] = part[block(t), cols(c)].astype(bf16)

    def launch(j, c):
        for way, goes, comes in ways:
            back = me if way == 0 else n - 1 - me

            @pl.when(goes)
            def _():
                transfer(way, raw, 0, 0, c).wait_send()

            @pl.when(goes & (j <= back))
            def _():
                transfer(way, raw, me - j if way == 0 else me + j, j, c).start()

            @pl.when(goes & (j > back))
            def _():
                t = n - j + me if way == 0 else j - n + me
                transfer(way, run, t + 1 if way == 0 else t, j, c).start()

    def take(j, c):
        for way, goes, comes in ways:
            back = me if way == 0 else n - 1 - me

            @pl.when(comes & (j <= back))
            def _():
                b = me - j if way == 0 else me + j
                absorb(b, c)
                if isinstance(c, int):
                    if c == CHUNKS - 1:
                        settle(b)
                else:
                    @pl.when(c == CHUNKS - 1)
                    def _():
                        settle(b)

    def step(j, c):
        arrive(j, c)
        prepare(j, c)
        launch(j, c)
        take(j, c)

    for l in loads[1:5]:
        l.wait()

    @pl.loop(0, heads // fold)
    def _(i):
        for p in range(fold):
            h = i * fold + p
            hs = pl.ds(pl.multiple_of(h * HEAD_DIM, HEAD_DIM), HEAD_DIM)
            x = grad[:, hs].astype(f32)
            turned = x * cos[...] - pltpu.roll(x, HEAD_DIM // 2, 1) * sin[...]
            plain = lax.rem(me * heads + h, GROUP) == GROUP - 1
            x = jnp.where(plain, x, turned)
            bg_ref[:, hs] = jnp.sum(x, axis=0, keepdims=True)
            low[:, hs] = x.astype(bf16)

    def backward(c):
        @pl.loop(0, per)
        def _(i):
            at = c * per + i
            w_copy(at).wait()

            @pl.when(at + DEPTH < tiles)
            def _():
                w_copy(at + DEPTH).start()

            k = pl.ds(pl.multiple_of(at * TILE_K, TILE_K), TILE_K)
            part[:, k] = lax.dot_general(
                low[...], w[k, :], (((1,), (1,)), ((), ())), preferred_element_type=f32
            )

    @pl.loop(0, CHUNKS)
    def _(c):
        backward(c)
        step(1, c)

    @pl.loop(0, CHUNKS)
    def _(c):
        absorb(me, c)
        tok[:, cols(c)] = raw[block(me), cols(c)]

    settle(me)

    @pl.loop(2, half)
    def _(j):
        @pl.loop(0, CHUNKS)
        def _(c):
            step(j, c)

    @pl.loop(0, CHUNKS)
    def _(c):
        arrive(half, c)
        prepare(half, c)

        @pl.when(c < CHUNKS - 1)
        def _():
            launch(half, c)

        take(half, c)


    def gain_add(source, at, t):
        scale = scale_ref[block(t), :]

        @pl.loop(0, depth // 1024)
        def _(i):
            for p in range(1024 // HEAD_DIM):
                k = pl.ds(pl.multiple_of(i * 1024 + p * HEAD_DIM, HEAD_DIM), HEAD_DIM)
                x = source[block(at), k].astype(f32) * raw[block(t), k].astype(f32) * scale
                total = x[:8]
                for r in range(8, rows, 8):
                    total = total + x[r:r + 8]
                gsum[:, k] += total

    gsum[...] = jnp.zeros_like(gsum)

    @pl.loop(0, n)
    def _(t):
        @pl.when((me - t < half) & (t - me < half))
        def _():
            gain_add(part, t, t)

    @pl.when(me >= half)
    def _():
        gain_add(run, me - half, me - half)

    @pl.when(me + half < n)
    def _():
        gain_add(run, me + half + 1, me + half)

    piece = depth // 16
    for i in range(16):
        gmine[i:i + 1, :] = jnp.sum(gsum[:, i * piece:(i + 1) * piece], axis=0, keepdims=True)

    def gain_copy(way):
        return pltpu.make_async_remote_copy(
            src_ref=gout.at[way],
            dst_ref=gin.at[way],
            send_sem=gsend_sem.at[way],
            recv_sem=grecv_sem.at[way],
            device_id=peer(way),
            device_id_type=MESH,
        )

    def relay(way):
        gain_copy(way).wait_recv()
        gout[way] = (gmine[...] + gin[way].astype(f32)).astype(bf16)
        gain_copy(way).start()

    for way, goes, comes in ways:
        @pl.when(goes & jnp.logical_not(comes))
        def _():
            gout[way] = gmine[...].astype(bf16)
            gain_copy(way).start()

    launch(half, CHUNKS - 1)

    @pl.loop(half + 1, n - 1)
    def _(j):
        @pl.loop(0, CHUNKS)
        def _(c):
            step(j, c)

    near = (me < half, me >= half)
    tile_n = 640 if width % 640 == 0 else HEAD_DIM
    tiles_n = width // tile_n

    def forward(c):
        @pl.loop(0, tiles_n)
        def _(i):
            ns = pl.ds(pl.multiple_of(i * tile_n, tile_n), tile_n)
            value = jnp.dot(held[:, cols(c)], w[cols(c), ns], preferred_element_type=f32)

            @pl.when(c == 0)
            def _():
                acc[:, ns] = value

            @pl.when(c > 0)
            def _():
                acc[:, ns] += value

    first, second = CHUNKS // 4, CHUNKS - 1
    @pl.loop(0, CHUNKS)
    def _(c):
        arrive(n - 1, c)
        prepare(n - 1, c)
        for way, goes, comes in ways:
            @pl.when(
                goes & comes & ((near[way] & (c == first)) | (near[1 - way] & (c == second)))
            )
            def _():
                relay(way)

        @pl.when(jnp.logical_not(patient & (c == CHUNKS - 1)))
        def _():
            launch(n - 1, c)

        take(n - 1, c)
        forward(c)

    @pl.loop(0, heads // fold)
    def _(i):
        for p in range(fold):
            h = i * fold + p
            hs = pl.ds(pl.multiple_of(h * HEAD_DIM, HEAD_DIM), HEAD_DIM)
            x = acc[:, hs] * scale_ref[...] + bias[:, hs]
            turned = x * cos[...] + pltpu.roll(x, HEAD_DIM // 2, 1) * sin[...]
            plain = lax.rem(me * heads + h, GROUP) == GROUP - 1
            qkv[:, hs] = jnp.where(plain, x, turned).astype(bf16)

    scale = scale_ref[block(me), :][:, :1]
    inner = jnp.zeros((rows, 1), f32)
    for c in range(CHUNKS):
        ks = slice(c * span, (c + 1) * span)
        if c == CHUNKS - 2:
            @pl.when(patient)
            def _():
                pl.delay(1600)
                launch(n - 1, CHUNKS - 1)

        if c == CHUNKS - 1:
            for way, goes, comes in ways:
                @pl.when(comes & jnp.logical_not(goes))
                def _():
                    gain_copy(way).wait_recv()

                @pl.when(comes)
                def _():
                    gmine[...] += gin[way].astype(f32)
            for i in range(16):
                gg_ref[:, i * piece:(i + 1) * piece] = gmine[i:i + 1, :]
        tgp[:, ks] = part[block(me), ks]
        for way, goes, comes in ways:
            @pl.when(comes)
            def _():
                slot = me + 1 - way
                transfer(way, run, slot, n - 1, c).wait_recv()
                tgp[:, ks] += run[block(slot), ks].astype(f32)

        scaled = tgp[:, ks] * gain[:, ks]
        inner = inner + jnp.sum(scaled * tok[:, ks].astype(f32), axis=1, keepdims=True)
        tgp[:, ks] = scaled * scale

    weight[...] = jnp.broadcast_to(scale * scale * scale * (inner / depth), weight.shape)

    for way, goes, comes in ways:
        @pl.when(goes)
        def _():
            gain_copy(way).wait_send()
            for c in range(CHUNKS):
                transfer(way, raw, 0, 0, c).wait_send()


def finish(qkv, tgp, tok, weight, gg, bg, qkv_h, tg_h, gg_h, bg_h, tg, sem):
    moves = ((qkv, qkv_h), (gg.at[0], gg_h), (bg.at[0], bg_h))
    copies = [pltpu.make_async_copy(src, dst, sem.at[i]) for i, (src, dst) in enumerate(moves)]
    for c in copies:
        c.start()
    factor = weight[:, :1]
    span = tg.shape[1] // PIECES
    for p in range(PIECES):
        ks = slice(p * span, (p + 1) * span)
        tg[:, ks] = tgp[:, ks] - tok[:, ks].astype(jnp.float32) * factor
        c = pltpu.make_async_copy(tg.at[:, ks], tg_h.at[:, ks], sem.at[3 + p])
        c.start()
        copies.append(c)
    for c in copies:
        c.wait()


def shards(n, tokens, norm_gain, qkv_weight, qkv_bias, qkv_grad):
    rows, depth = tokens.shape
    every, width = qkv_grad.shape
    cosine, sine = rope_tables(every, rows, SEQ_LEN // n)
    bf16, f32 = jnp.bfloat16, jnp.float32
    dma = pltpu.SemaphoreType.DMA
    hbm = pl.BlockSpec(memory_space=pl.ANY)
    vmem = pl.BlockSpec(memory_space=pltpu.VMEM)
    results = pl.pallas_call(
        functools.partial(kernel, n),
        out_shape=(
            pltpu.VMEM((every, width), bf16),
            pltpu.VMEM((rows, depth), f32),
            pltpu.VMEM((rows, depth), bf16),
            pltpu.VMEM((rows, HEAD_DIM), f32),
            pltpu.VMEM((1, depth), f32),
            pltpu.VMEM((1, width), f32),
        ),
        in_specs=[hbm] * 6,
        out_specs=[vmem] * 6,
        scratch_shapes=[
            pltpu.VMEM((every, depth), bf16),
            pltpu.VMEM((1, depth), f32),
            pltpu.VMEM((depth, width), bf16),
            pltpu.VMEM((1, width), f32),
            pltpu.VMEM((every, width), bf16),
            pltpu.VMEM((2 * every, HEAD_DIM), f32),
            pltpu.VMEM((every, width), bf16),
            pltpu.VMEM((every, depth), f32),
            pltpu.VMEM((every, depth), bf16),
            pltpu.VMEM((every + rows, depth), bf16),
            pltpu.VMEM((every, width), f32),
            pltpu.VMEM((every, HEAD_DIM), f32),
            pltpu.VMEM((every, HEAD_DIM), f32),
            pltpu.VMEM((8, depth), f32),
            pltpu.VMEM((16, depth // 16), f32),
            pltpu.VMEM((2, 16, depth // 16), bf16),
            pltpu.VMEM((2, 16, depth // 16), bf16),
            dma((5,)),
            dma((DEPTH,)),
            dma((2, CHUNKS)),
            dma((2, 2, CHUNKS)),
            dma((2,)),
            dma((2,)),
            pltpu.SemaphoreType.REGULAR,
        ],
        compiler_params=pltpu.CompilerParams(
            collective_id=0, has_side_effects=True, vmem_limit_bytes=60000000
        ),
        cost_estimate=pl.CostEstimate(
            flops=4 * every * depth * width, bytes_accessed=2 * depth * width, transcendentals=0
        ),
    )(
        tokens, norm_gain, qkv_weight, qkv_bias, qkv_grad,
        jnp.asarray(np.concatenate([cosine, sine])),
    )
    return pl.pallas_call(
        finish,
        out_shape=(
            jax.ShapeDtypeStruct((every, width), bf16),
            jax.ShapeDtypeStruct((rows, depth), f32),
            jax.ShapeDtypeStruct((depth,), f32),
            jax.ShapeDtypeStruct((width,), f32),
        ),
        in_specs=[vmem] * 6,
        out_specs=[hbm] * 4,
        scratch_shapes=[pltpu.VMEM((rows, depth), f32), dma((3 + PIECES,))],
        compiler_params=pltpu.CompilerParams(vmem_limit_bytes=3 << 20),
    )(*results)


def solution(mesh):
    in_specs = (P(("dp", "mp"), None), P(), P(None, "mp"), P("mp"), P("dp", "mp"))
    out_specs = (P("dp", "mp"), P(("dp", "mp"), None), P("dp"), P(("dp", "mp")))
    body = functools.partial(shards, mesh.shape["mp"])
    return jax.shard_map(body, mesh=mesh, in_specs=in_specs, out_specs=out_specs, check_vma=False)
```
